32 devices in a mesh: gx: 8 (over y, x, core), gy: 4 (over z).
Axes of the slice: x: 2, y: 2, z: 4, core: 2. Of those that a mesh axis runs over, the one named last changes fastest.
Arguments:
- rhs_conc: float32 [16, 64, 2048], P('gx', 'gy'), may hold values from -60 to 60
- rhs_pots: float32 [16, 64, 33], P('gx', 'gy'), may hold values from -60 to 60
- diffusion: float32 [16, 64, 32], P('gx', 'gy'), may hold values from 0.05 to 5
- exchange: float32 [16, 64, 32], P('gx', 'gy'), may hold values from 0.2 to 4
- slope: float32 [16, 64, 32], P('gx', 'gy'), may hold values from 0.1 to 1
Outputs:
- sol_conc: float32 [16, 64, 2048], P('gx', 'gy')
- sol_pots: float32 [16, 64, 33], P('gx', 'gy')
The draws below stay inside these ranges and needn't reach their ends.
All inputs are finite; a program needn't handle non-finite values.
Results may differ from the reference program's by a relative error of at most 0.0003.
Values sent between devices are 32-bit elements; how exact they have to be, the bound alone decides.
A program may use at most 64 MiB of HBM per device.

```python
import math
import jax
import jax.numpy as jnp
from jax import lax

NE = 32
NR = 64
ITERS = 10
NX = 16
NY = 64


def column_scale(key):
    scale_key = jax.random.fold_in(key, 7)
    row_place = jnp.arange(NX, dtype=jnp.float32)[:, None] / max(NX - 1, 1)
    spread_field = jnp.exp(jax.random.uniform(scale_key, (NX, NY), jnp.float32) * math.log(10.0))
    scale_field = spread_field * jnp.exp(row_place * math.log(3.0))
    return 0.25 * scale_field


def draw_values(key, width):
    values = jnp.clip(jax.random.normal(key, (NX, NY, width), jnp.float32), -5.0, 5.0)
    return values


def draw_rhs_conc(key, part):
    scale_field = column_scale(key)
    values = draw_values(jax.random.fold_in(key, 11), NE * NR)
    return scale_field[:, :, None] * values


def draw_rhs_pots(key, part):
    scale_field = column_scale(key)
    values = draw_values(jax.random.fold_in(key, 13), NE + 1)
    return scale_field[:, :, None] * values


def levels(stream_key, extent, cuts, low, high):
    def one(position, blocks):
        heights = jax.random.uniform(jax.random.fold_in(jax.random.fold_in(stream_key, 6), position), (blocks,), jnp.float32, low / len(cuts), high / len(cuts))
        return jnp.repeat(jnp.exp(heights), extent[position] // blocks).reshape((-1,) + (1,) * (len(extent) - position - 1))

    gain = one(*cuts[0])
    for cut in cuts[1:]:
        gain = gain * one(*cut)
    return gain


def setup_inputs(seed: int = 0) -> dict:
    seeds = jax.random.split(jax.random.key(seed), 6)
    rhs_conc = draw_rhs_conc(jax.random.fold_in(seeds[5], 71), 0)
    rhs_pots = draw_rhs_pots(jax.random.fold_in(seeds[5], 71), 0)
    diffusion = jnp.clip(jnp.exp(math.log(5.0) - 4.6051702 * jax.random.uniform(seeds[2], (NX, NY, NE), jnp.float32) ** levels(seeds[2], (NX, NY, NE), ((0, 8), (1, 4)), -0.2, 0.2)), 0.05, 5.0)
    exchange = jnp.clip(jnp.exp(math.log(4.0) - 2.9957323 * jax.random.uniform(seeds[3], (NX, NY, NE), jnp.float32) ** levels(seeds[3], (NX, NY, NE), ((0, 8), (1, 4)), -0.2, 0.2)), 0.2, 4.0)
    slope = jnp.clip(0.1 + 0.9 * jax.random.uniform(seeds[4], (NX, NY, NE), jnp.float32) ** levels(seeds[4], (NX, NY, NE), ((0, 8), (1, 4)), -0.2, 0.2), 0.1, 1.0)
    return dict(rhs_conc=rhs_conc, rhs_pots=rhs_pots, diffusion=diffusion, exchange=exchange, slope=slope)


node_cond = 1.0
plane_cond = 0.5
collector_cond = 2.0
epsilon = 1e-06

def mirror_laplace(values):
    inner = jnp.concatenate([values[..., :1], values[..., :-1]], axis=-1)
    outer = jnp.concatenate([values[..., 1:], values[..., -1:]], axis=-1)
    return 2.0 * values - inner - outer

def local_operator(conc, padded, diffusion, exchange, slope):
    nodes = exchange.shape[2]
    shell_count = conc.shape[2] // nodes
    shells = conc.reshape(conc.shape[0], conc.shape[1], nodes, shell_count)
    center = padded[1:-1, 1:-1]
    lateral = 4.0 * center - padded[2:, 1:-1] - padded[:-2, 1:-1] - padded[1:-1, 2:] - padded[1:-1, :-2]
    node_pot = center[..., :nodes]
    collector = center[..., nodes]
    current = exchange * (node_pot - collector[..., None])
    surface = shells[..., shell_count - 1]
    surface_flag = (lax.broadcasted_iota(jnp.int32, (shell_count,), 0) == shell_count - 1).astype(jnp.float32)
    new_shells = shells + diffusion[..., None] * mirror_laplace(shells) + current[..., None] * surface_flag
    new_nodes = node_cond * mirror_laplace(node_pot) + current - slope * surface + plane_cond * lateral[..., :nodes]
    new_collector = collector_cond * lateral[..., nodes] - lax.optimization_barrier(jnp.mean(current, axis=-1))
    return (new_shells.reshape(conc.shape), jnp.concatenate([new_nodes, new_collector[..., None]], axis=-1))

def least_squares(columns, start_norm):
    count = len(columns)
    target = [start_norm] + [jnp.zeros_like(start_norm) for step in range(count)]
    cosines = []
    sines = []
    upper_rows = []
    for step in range(count):
        entries = list(columns[step])
        for row in range(step):
            first = cosines[row] * entries[row] + sines[row] * entries[row + 1]
            second = cosines[row] * entries[row + 1] - sines[row] * entries[row]
            entries[row] = first
            entries[row + 1] = second
        radius = jnp.sqrt(entries[step] * entries[step] + entries[step + 1] * entries[step + 1])
        cosine = entries[step] / radius
        sine = entries[step + 1] / radius
        entries[step] = radius
        cosines.append(cosine)
        sines.append(sine)
        lead = target[step]
        target[step] = cosine * lead
        target[step + 1] = -sine * lead
        upper_rows.append(entries[:step + 1])
    weights = [None] * count
    for row in range(count - 1, -1, -1):
        total = target[row]
        for later in range(row + 1, count):
            total = total - upper_rows[later][row] * weights[later]
        weights[row] = total / upper_rows[row][row]
    return weights

def apply_operator(conc, pots, diffusion, exchange, slope):
    padded = jnp.pad(pots, ((1, 1), (1, 1), (0, 0)))
    return local_operator(conc, padded, diffusion, exchange, slope)

def reference(rhs_conc, rhs_pots, diffusion, exchange, slope):
    start_norm = jnp.sqrt(jnp.sum(rhs_conc * rhs_conc) + jnp.sum(rhs_pots * rhs_pots) + epsilon)
    basis = [(rhs_conc / start_norm, rhs_pots / start_norm)]
    columns = []
    for step in range(ITERS):
        image_conc, image_pots = apply_operator(basis[step][0], basis[step][1], diffusion, exchange, slope)
        coeffs = [jnp.sum(vector[0] * image_conc) + jnp.sum(vector[1] * image_pots) for vector in basis]
        rest_conc, rest_pots = (image_conc, image_pots)
        for row in range(step + 1):
            rest_conc = rest_conc - coeffs[row] * basis[row][0]
            rest_pots = rest_pots - coeffs[row] * basis[row][1]
        height = jnp.sqrt(jnp.sum(rest_conc * rest_conc) + jnp.sum(rest_pots * rest_pots) + epsilon)
        basis.append((rest_conc / height, rest_pots / height))
        columns.append(coeffs + [height])
    weights = least_squares(columns, start_norm)
    sol_conc = weights[0] * basis[0][0]
    sol_pots = weights[0] * basis[0][1]
    for step in range(1, ITERS):
        sol_conc = sol_conc + weights[step] * basis[step][0]
        sol_pots = sol_pots + weights[step] * basis[step][1]
    return (sol_conc, sol_pots)
```

```python
import functools

import jax
import jax.numpy as jnp
from jax import lax
from jax.experimental import pallas as pl
from jax.experimental.pallas import tpu as pltpu
from jax.sharding import PartitionSpec as P

ITERS = 10
LANES = 128
CHUNK = 16

node_cond = 1.0
plane_cond = 0.5
collector_cond = 2.0
epsilon = 1e-06
MESH = pl.DeviceIdType.MESH


def cycle(
    sizes,
    conc_ref,
    pots_ref,
    diff_ref,
    exch_ref,
    slope_ref,
    sol_conc_ref,
    sol_pots_ref,
    turned,
    basis,
    image,
    edges,
    halos,
    rows,
    sent_rows,
    edge_send,
    edge_recv,
    row_send,
    row_recv,
):
    nx, ny = sizes
    count = nx * ny
    cx, cy = conc_ref.shape[0], conc_ref.shape[1]
    cells = cx * cy
    nodes = exch_ref.shape[2]
    shells = conc_ref.shape[2] // nodes
    groups = LANES // cells
    subs = nodes // groups
    mx = lax.axis_index("gx")
    my = lax.axis_index("gy")
    me = mx * ny + my

    def peers(act):
        if count <= 32:
            for dx in range(nx - 1, -1, -1):
                for dy in range(ny - 1, -1, -1):
                    if dx or dy:
                        act(lax.rem(mx + dx, nx), lax.rem(my + dy, ny))
        else:

            def one(p, carry):
                other = lax.rem(me + p, count)
                act(lax.div(other, ny), lax.rem(other, ny))
                return carry

            lax.fori_loop(1, count, one, 0)

    barrier = pltpu.get_barrier_semaphore()
    peers(
        lambda px, py: pl.semaphore_signal(
            barrier, inc=1, device_id={"gx": px, "gy": py}, device_id_type=MESH
        )
    )

    def fold_nodes(block):
        flat = block.reshape(cells, block.shape[2])
        return flat.T

    def node_register(flat_t):
        return jnp.concatenate(
            [flat_t[g * subs : (g + 1) * subs, :] for g in range(groups)], axis=1
        )

    diff = node_register(fold_nodes(diff_ref[...]))
    exch = node_register(fold_nodes(exch_ref[...]))
    slope = node_register(fold_nodes(slope_ref[...]))
    pots_t = fold_nodes(pots_ref[...])
    pot = node_register(pots_t)
    vol_row = pots_t[nodes : nodes + 1, :]
    vol = jnp.broadcast_to(jnp.concatenate([vol_row] * groups, axis=1), (subs, LANES))

    span = subs * shells
    for x in range(cx):
        for g in range(groups):
            edge_row = g * cells + x * cy
            turned[edge_row : edge_row + cy, :] = conc_ref[x, :, g * span : (g + 1) * span]
    image_flat = turned[...].T
    turned_t = image_flat.reshape(subs, shells, LANES)
    for s in range(subs):
        basis[0, 1 : shells + 1, s, :] = turned_t[s]

    lane = lax.broadcasted_iota(jnp.int32, (subs, LANES), 1)
    sub = lax.broadcasted_iota(jnp.int32, (subs, LANES), 0)
    group = lane // cells
    cell = lane % cells
    cell_x = cell // cy
    cell_y = cell % cy
    single = ((sub == 0) & (group == 0)).astype(jnp.float32)
    first_sub, last_sub = sub == 0, sub == subs - 1
    first_group, last_group = group == 0, group == groups - 1
    inside_low_x, inside_high_x = cell_x > 0, cell_x < cx - 1
    inside_low_y, inside_high_y = cell_y > 0, cell_y < cy - 1
    zero = jnp.zeros((subs, LANES), jnp.float32)
    has = [mx > 0, mx < nx - 1, my > 0, my < ny - 1]

    def roll(value, shift, axis=1):
        shift = shift % value.shape[axis]
        return pltpu.roll(value, shift, axis) if shift else value

    def inner_plane(p):
        return (
            4.0 * p
            - jnp.where(inside_low_x, roll(p, cy), zero)
            - jnp.where(inside_high_x, roll(p, -cy), zero)
            - jnp.where(inside_low_y, roll(p, 1), zero)
            - jnp.where(inside_high_y, roll(p, -1), zero)
        )

    def edge_sum(slot, member):
        low_x = roll(halos[slot, 0, member], -(cx - 1) * cy)
        high_x = roll(halos[slot, 1, member], (cx - 1) * cy)
        low_y = roll(halos[slot, 2, member], -(cy - 1))
        high_y = roll(halos[slot, 3, member], cy - 1)
        return (
            jnp.where(~inside_low_x & has[0], low_x, zero)
            + jnp.where(~inside_high_x & has[1], high_x, zero)
            + jnp.where(~inside_low_y & has[2], low_y, zero)
            + jnp.where(~inside_high_y & has[3], high_y, zero)
        )

    def node_mirror(p):
        low = roll(p, 1, 0)
        inner = jnp.where(first_sub, jnp.where(first_group, p, roll(low, cells)), low)
        high = roll(p, -1, 0)
        outer = jnp.where(last_sub, jnp.where(last_group, p, roll(high, -cells)), high)
        return 2.0 * p - inner - outer

    def node_mean(value):
        total = jnp.broadcast_to(jnp.sum(value, axis=0, keepdims=True), (subs, LANES))
        shift = cells
        while shift < LANES:
            total = total + roll(total, shift)
            shift *= 2
        return total * (1.0 / nodes)

    def edge_copies(slot):
        copies = []
        targets = [
            (lax.rem(mx + 1, nx), my),
            (lax.rem(mx + nx - 1, nx), my),
            (mx, lax.rem(my + 1, ny)),
            (mx, lax.rem(my + ny - 1, ny)),
        ]
        for k, (px, py) in enumerate(targets):
            copies.append(
                pltpu.make_async_remote_copy(
                    src_ref=edges.at[slot],
                    dst_ref=halos.at[slot, k],
                    send_sem=edge_send.at[slot, k],
                    recv_sem=edge_recv.at[slot, k],
                    device_id={"gx": px, "gy": py},
                    device_id_type=MESH,
                )
            )
        return copies

    def pots_image(p, v, ep, ev, surface):
        current = exch * (p - v)
        new_p = (
            node_cond * node_mirror(p)
            + current
            - slope * surface
            + plane_cond * (inner_plane(p) - ep)
        )
        new_v = collector_cond * (inner_plane(v) - ev) - node_mean(current)
        return new_p, new_v, current

    def image_and_dots(step, current, starts):
        def part(at, carry, last):
            here = basis[step, pl.ds(at + 1, CHUNK)]
            low = basis[step, pl.ds(at, CHUNK)]
            high = basis[step, pl.ds(at + 2, CHUNK)]
            new = here + diff[None] * (2.0 * here - low - high)
            if last:
                new = jnp.concatenate([new[:-1], new[-1:] + current[None]], axis=0)
            image[pl.ds(at, CHUNK)] = new
            out = []
            for i in range(step + 1):
                other = here if i == step else basis[i, pl.ds(at + 1, CHUNK)]
                out.append(carry[i] + jnp.sum(other * new, axis=0))
            out.append(carry[step + 1] + jnp.sum(new * new, axis=0))
            if step == 0:
                out.append(carry[2] + jnp.sum(here * here, axis=0))
            return tuple(out)

        parts = shells // CHUNK
        carry = lax.fori_loop(
            0, parts - 1, lambda c, carry: part(c * CHUNK, carry, False), tuple(starts)
        )
        return part((parts - 1) * CHUNK, carry, True)

    def row_copy(step, px, py):
        return pltpu.make_async_remote_copy(
            src_ref=sent_rows.at[step],
            dst_ref=rows.at[step, me],
            send_sem=row_send.at[step],
            recv_sem=row_recv.at[step],
            device_id={"gx": px, "gy": py},
            device_id_type=MESH,
        )

    def send_dots(step, dots):
        padded = -(-len(dots) // 8) * 8
        stacked = [jnp.sum(d, axis=0, keepdims=True) for d in dots]
        stacked += [zero[:1]] * (padded - len(dots))
        tall = jnp.sum(jnp.concatenate(stacked, axis=0), axis=1, keepdims=True)
        at_row = lax.broadcasted_iota(jnp.int32, (padded, LANES), 0)
        at_lane = lax.broadcasted_iota(jnp.int32, (padded, LANES), 1)
        row = jnp.sum(jnp.where(at_row == at_lane, tall, 0.0), axis=0, keepdims=True)
        sent_rows[step] = row
        rows[step, me] = row
        peers(lambda px, py: row_copy(step, px, py).start())

    def wait_rows(step):
        part = rows.at[step, pl.ds(0, count - 1)]
        pltpu.make_async_copy(part, part, row_recv.at[step]).wait()

    def take_dots(step, wanted):
        total = jnp.sum(rows[step], axis=0)
        return [jnp.broadcast_to(total[:, k : k + 1], (subs, LANES)) for k in range(wanted)]

    def pad_ends(step):
        basis[step, 0] = basis[step, 1]
        basis[step, shells + 1] = basis[step, shells]

    pad_ends(0)
    edges[0, 0] = pot
    edges[0, 1] = vol
    pl.semaphore_wait(barrier, count - 1)
    started = edge_copies(0)
    for copy in started:
        copy.start()
    pending = list(started)

    for copy in started:
        copy.wait_recv()
    vecs = [(pot, vol, edge_sum(0, 0), edge_sum(0, 1))]
    cosines, sines, uppers, target = [], [], [], []
    heights = None
    for step in range(ITERS):
        p, v, ep, ev = vecs[step]
        new_p, new_v, current = pots_image(p, v, ep, ev, basis[step, shells])
        more = step < ITERS - 1
        if more:
            edges[step + 1, 0] = new_p
            edges[step + 1, 1] = new_v
            started = edge_copies(step + 1)
            for copy in started:
                copy.start()
            pending += started
        if step > 0:
            pad_ends(step)
        new_v_once = new_v * single
        starts = [vecs[i][0] * new_p + vecs[i][1] * new_v_once for i in range(step + 1)]
        starts.append(new_p * new_p + new_v * new_v_once)
        if step == 0:
            starts.append(pot * pot + vol * (vol * single))
        dots = image_and_dots(step, current, starts)
        send_dots(step, dots)
        wait_rows(step)
        sums = take_dots(step, len(dots))
        scale = None
        if step == 0:
            beta = jnp.sqrt(sums[2] + epsilon)
            scale = 1.0 / beta
            coeffs = [sums[0] * scale * scale]
            square = sums[1] * scale * scale
            target.append(beta)
        else:
            coeffs = list(sums[: step + 1])
            square = sums[step + 1]
        rest = square
        taken = coeffs[0] * coeffs[0]
        for h in coeffs[1:]:
            taken = taken + h * h
        height = jnp.sqrt(square - taken + epsilon)
        inverse = 1.0 / height
        if more:
            for copy in started:
                copy.wait_recv()
            if step == 0:
                vecs[0] = tuple(m * scale for m in vecs[0])
            new = [new_p, new_v, edge_sum(step + 1, 0), edge_sum(step + 1, 1)]
            for k in range(4):
                u = new[k] if step else new[k] * scale
                for i in range(step + 1):
                    u = u - coeffs[i] * vecs[i][k]
                new[k] = u * inverse
            vecs.append(tuple(new))

            def advance(c, carry):
                at = c * CHUNK
                u = image[pl.ds(at, CHUNK)]
                if step == 0:
                    first = basis[0, pl.ds(at + 1, CHUNK)] * scale[None]
                    basis[0, pl.ds(at + 1, CHUNK)] = first
                    u = u * scale[None] - coeffs[0][None] * first
                else:
                    for i in range(step + 1):
                        u = u - coeffs[i][None] * basis[i, pl.ds(at + 1, CHUNK)]
                basis[step + 1, pl.ds(at + 1, CHUNK)] = u * inverse[None]
                return carry

            lax.fori_loop(0, shells // CHUNK, advance, 0)
        entries = coeffs + [height]
        for row in range(step):
            first = cosines[row] * entries[row] + sines[row] * entries[row + 1]
            second = cosines[row] * entries[row + 1] - sines[row] * entries[row]
            entries[row] = first
            entries[row + 1] = second
        radius = jnp.sqrt(entries[step] * entries[step] + entries[step + 1] * entries[step + 1])
        cosine = entries[step] / radius
        sine = entries[step + 1] / radius
        entries[step] = radius
        cosines.append(cosine)
        sines.append(sine)
        lead = target[step]
        target[step] = cosine * lead
        target.append(-sine * lead)
        uppers.append(entries[: step + 1])

    weights = [None] * ITERS
    for row in range(ITERS - 1, -1, -1):
        total = target[row]
        for later in range(row + 1, ITERS):
            total = total - uppers[later][row] * weights[later]
        weights[row] = total / uppers[row][row]

    sol_p = weights[0] * vecs[0][0]
    sol_v = weights[0] * vecs[0][1]
    for i in range(1, ITERS):
        sol_p = sol_p + weights[i] * vecs[i][0]
        sol_v = sol_v + weights[i] * vecs[i][1]

    def combine(c, carry):
        at = c * CHUNK
        total = weights[0][None] * basis[0, pl.ds(at + 1, CHUNK)]
        for i in range(1, ITERS):
            total = total + weights[i][None] * basis[i, pl.ds(at + 1, CHUNK)]
        image[pl.ds(at, CHUNK)] = total
        return carry

    lax.fori_loop(0, shells // CHUNK, combine, 0)
    flat = jnp.concatenate([image[:, s, :] for s in range(subs)], axis=0)
    turned[...] = flat.T
    for x in range(cx):
        for g in range(groups):
            edge_row = g * cells + x * cy
            sol_conc_ref[x, :, g * span : (g + 1) * span] = turned[edge_row : edge_row + cy, :]
    flat_p = jnp.concatenate(
        [sol_p[:, g * cells : (g + 1) * cells] for g in range(groups)] + [sol_v[:1, :cells]], axis=0
    )
    sol_pots_ref[...] = flat_p.T.reshape(cx, cy, nodes + 1)

    for copy in pending:
        copy.wait_send()
    for step in range(ITERS):
        part = rows.at[step, pl.ds(0, count - 1)]
        pltpu.make_async_copy(part, part, row_send.at[step]).wait()


def solution(mesh):
    sizes = (mesh.shape["gx"], mesh.shape["gy"])
    count = sizes[0] * sizes[1]

    def shards(rhs_conc, rhs_pots, diffusion, exchange, slope):
        cells = rhs_conc.shape[0] * rhs_conc.shape[1]
        nodes = exchange.shape[2]
        shells = rhs_conc.shape[2] // nodes
        groups = LANES // cells
        subs = nodes // groups
        vmem = pl.BlockSpec(memory_space=pltpu.VMEM)
        return pl.pallas_call(
            functools.partial(cycle, sizes),
            out_shape=(
                jax.ShapeDtypeStruct(rhs_conc.shape, jnp.float32),
                jax.ShapeDtypeStruct(rhs_pots.shape, jnp.float32),
            ),
            in_specs=[vmem] * 5,
            out_specs=(vmem, vmem),
            scratch_shapes=[
                pltpu.VMEM((LANES, subs * shells), jnp.float32),
                pltpu.VMEM((ITERS, shells + 2, subs, LANES), jnp.float32),
                pltpu.VMEM((shells, subs, LANES), jnp.float32),
                pltpu.VMEM((ITERS, 2, subs, LANES), jnp.float32),
                pltpu.VMEM((ITERS, 4, 2, subs, LANES), jnp.float32),
                pltpu.VMEM((ITERS, count, 1, LANES), jnp.float32),
                pltpu.VMEM((ITERS, 1, LANES), jnp.float32),
                pltpu.SemaphoreType.DMA((ITERS, 4)),
                pltpu.SemaphoreType.DMA((ITERS, 4)),
                pltpu.SemaphoreType.DMA((ITERS,)),
                pltpu.SemaphoreType.DMA((ITERS,)),
            ],
            compiler_params=pltpu.CompilerParams(collective_id=0, has_side_effects=True),
        )(rhs_conc, rhs_pots, diffusion, exchange, slope)

    spec = P("gx", "gy", None)
    return jax.shard_map(
        shards,
        mesh=mesh,
        in_specs=(spec,) * 5,
        out_specs=(spec, spec),
        check_vma=False,
    )
```

```python
import functools

import jax
import jax.numpy as jnp
from jax import lax
from jax.experimental import pallas as pl
from jax.experimental.pallas import tpu as pltpu
from jax.sharding import PartitionSpec as P

ITERS = 10
LANES = 128
CHUNK = 16

node_cond = 1.0
plane_cond = 0.5
collector_cond = 2.0
epsilon = 1e-06
first_shift = 3.0
MESH = pl.DeviceIdType.MESH


def add(terms):
    terms = [t for t in terms if t is not None]
    while len(terms) > 1:
        pairs = [terms[k] + terms[k + 1] for k in range(0, len(terms) - 1, 2)]
        terms = pairs + ([terms[-1]] if len(terms) % 2 else [])
    return terms[0]


def two_columns(last, upper, gram, along1, along2, z11, z12, z22, shift, root, ramp):
    span = range(last + 1)

    def images_of_rest(cu):
        out = []
        for k in span:
            terms = [cu[i] * upper[i][k] for i in range(max(k - 1, 0), last)]
            if k == last:
                terms.append(cu[last] * shift)
            out.append(add(terms))
        return out

    h = [along1[i] + shift * gram[i][last] for i in span]
    cu = [-h[i] for i in span]
    cu[last] = shift - h[last]
    gu = [h[i] - add([h[k] * gram[i][k] for k in span]) for i in span]
    g1 = z11 + shift * along1[last] - add([h[k] * along1[k] for k in span])
    g2 = z12 + shift * along2[last] - add([h[k] * along2[k] for k in span])
    square = add([cu[i] * gu[i] for i in span] + [g1])
    height, inverse = root(ramp(square))
    col1 = h + [height]
    first = [c * inverse for c in cu]
    near = [g * inverse for g in gu]
    near1, near2 = g1 * inverse, g2 * inverse
    near_self = ramp(square) * inverse * inverse

    cw = [c * inverse for c in images_of_rest(cu)]
    c1 = (cu[last] + shift) * inverse
    c2 = inverse
    g = [
        add([cw[k] * gram[i][k] for k in span] + [c1 * along1[i], c2 * along2[i]]) for i in span
    ]
    g1 = add([cw[k] * along1[k] for k in span] + [c1 * z11, c2 * z12])
    g2 = add([cw[k] * along2[k] for k in span] + [c1 * z12, c2 * z22])
    h = list(g)
    top = add([first[i] * g[i] for i in span] + [inverse * g1])
    cu = [cw[i] - h[i] - top * first[i] for i in span]
    c1 = c1 - top * inverse
    gu = [g[i] - add([h[k] * gram[i][k] for k in span] + [top * near[i]]) for i in span]
    g1 = g1 - add([h[k] * along1[k] for k in span] + [top * near1])
    g2 = g2 - add([h[k] * along2[k] for k in span] + [top * near2])
    square = add([cu[i] * gu[i] for i in span] + [c1 * g1, c2 * g2])
    height, inverse2 = root(ramp(square))
    col2 = h + [top, height]
    second = ([c * inverse2 for c in cu], c1 * inverse2, c2 * inverse2)

    def next_image(new_shift):
        cq, d1, d2 = second
        out = images_of_rest(cq)
        out = [out[k] - new_shift * cq[k] for k in span]
        e1 = cq[last] + d1 * (shift - new_shift)
        e2 = d1 + d2 * (shift - new_shift)
        return out, e1, e2, d2

    gram = [list(gram[i]) + [near[i], gu[i] * inverse2] for i in span]
    cross = add([first[i] * gu[i] for i in span] + [inverse * g1]) * inverse2
    gram.append([gram[i][last + 1] for i in span] + [near_self, cross])
    gram.append([gram[i][last + 2] for i in span] + [cross, ramp(square) * inverse2 * inverse2])
    return col1, col2, (first, inverse), second, next_image, gram


def cycle(
    sizes,
    conc_ref,
    pots_ref,
    diff_ref,
    exch_ref,
    slope_ref,
    sol_conc_ref,
    sol_pots_ref,
    turned,
    basis,
    images,
    edges,
    halos,
    rows,
    sent_rows,
    edge_send,
    edge_recv,
    row_send,
    row_recv,
):
    nx, ny = sizes
    count = nx * ny
    cx, cy = conc_ref.shape[0], conc_ref.shape[1]
    cells = cx * cy
    nodes = exch_ref.shape[2]
    shells = conc_ref.shape[2] // nodes
    groups = LANES // cells
    subs = nodes // groups
    mx = lax.axis_index("gx")
    my = lax.axis_index("gy")
    me = mx * ny + my

    def peers(act):
        if count <= 32:
            for dx in range(nx - 1, -1, -1):
                for dy in range(ny - 1, -1, -1):
                    if dx or dy:
                        act(lax.rem(mx + dx, nx), lax.rem(my + dy, ny))
        else:

            def one(p, carry):
                other = lax.rem(me + p, count)
                act(lax.div(other, ny), lax.rem(other, ny))
                return carry

            lax.fori_loop(1, count, one, 0)

    barrier = pltpu.get_barrier_semaphore()
    peers(
        lambda px, py: pl.semaphore_signal(
            barrier, inc=1, device_id={"gx": px, "gy": py}, device_id_type=MESH
        )
    )

    def fold_nodes(block):
        flat = block.reshape(cells, block.shape[2])
        return flat.T

    def node_register(flat_t):
        return jnp.concatenate(
            [flat_t[g * subs : (g + 1) * subs, :] for g in range(groups)], axis=1
        )

    diff = node_register(fold_nodes(diff_ref[...]))
    exch = node_register(fold_nodes(exch_ref[...]))
    slope = node_register(fold_nodes(slope_ref[...]))
    pots_t = fold_nodes(pots_ref[...])
    pot = node_register(pots_t)
    vol_row = pots_t[nodes : nodes + 1, :]
    vol = jnp.broadcast_to(jnp.concatenate([vol_row] * groups, axis=1), (subs, LANES))

    span = subs * shells
    for x in range(cx):
        for g in range(groups):
            edge_row = g * cells + x * cy
            turned[edge_row : edge_row + cy, :] = conc_ref[x, :, g * span : (g + 1) * span]
    turned_t = turned[...].T.reshape(subs, shells, LANES)
    for s in range(subs):
        images[2, 1 : shells + 1, s, :] = turned_t[s]

    lane = lax.broadcasted_iota(jnp.int32, (subs, LANES), 1)
    sub = lax.broadcasted_iota(jnp.int32, (subs, LANES), 0)
    group = lane // cells
    cell = lane % cells
    cell_x = cell // cy
    cell_y = cell % cy
    single = ((sub == 0) & (group == 0)).astype(jnp.float32)
    first_sub, last_sub = sub == 0, sub == subs - 1
    first_group, last_group = group == 0, group == groups - 1
    inside_low_x, inside_high_x = cell_x > 0, cell_x < cx - 1
    inside_low_y, inside_high_y = cell_y > 0, cell_y < cy - 1
    zero = jnp.zeros((subs, LANES), jnp.float32)
    has = [mx > 0, mx < nx - 1, my > 0, my < ny - 1]

    def roll(value, shift, axis=1):
        shift = shift % value.shape[axis]
        return pltpu.roll(value, shift, axis) if shift else value

    def inner_plane(p):
        return (
            4.0 * p
            - jnp.where(inside_low_x, roll(p, cy), zero)
            - jnp.where(inside_high_x, roll(p, -cy), zero)
            - jnp.where(inside_low_y, roll(p, 1), zero)
            - jnp.where(inside_high_y, roll(p, -1), zero)
        )

    def edge_sum(slot, member):
        low_x = roll(halos[slot, 0, member], -(cx - 1) * cy)
        high_x = roll(halos[slot, 1, member], (cx - 1) * cy)
        low_y = roll(halos[slot, 2, member], -(cy - 1))
        high_y = roll(halos[slot, 3, member], cy - 1)
        return (
            jnp.where(~inside_low_x & has[0], low_x, zero)
            + jnp.where(~inside_high_x & has[1], high_x, zero)
            + jnp.where(~inside_low_y & has[2], low_y, zero)
            + jnp.where(~inside_high_y & has[3], high_y, zero)
        )

    def node_mirror(p):
        low = roll(p, 1, 0)
        inner = jnp.where(first_sub, jnp.where(first_group, p, roll(low, cells)), low)
        high = roll(p, -1, 0)
        outer = jnp.where(last_sub, jnp.where(last_group, p, roll(high, -cells)), high)
        return 2.0 * p - inner - outer

    def node_mean(value):
        total = jnp.broadcast_to(jnp.sum(value, axis=0, keepdims=True), (subs, LANES))
        shift = cells
        while shift < LANES:
            total = total + roll(total, shift)
            shift *= 2
        return total * (1.0 / nodes)

    def edge_copies(slot):
        copies = []
        targets = [
            (lax.rem(mx + 1, nx), my),
            (lax.rem(mx + nx - 1, nx), my),
            (mx, lax.rem(my + 1, ny)),
            (mx, lax.rem(my + ny - 1, ny)),
        ]
        for k, (px, py) in enumerate(targets):
            copies.append(
                pltpu.make_async_remote_copy(
                    src_ref=edges.at[slot],
                    dst_ref=halos.at[slot, k],
                    send_sem=edge_send.at[slot, k],
                    recv_sem=edge_recv.at[slot, k],
                    device_id={"gx": px, "gy": py},
                    device_id_type=MESH,
                )
            )
        return copies

    def pots_image(vec, surface, shift):
        p, v, ep, ev = vec
        current = exch * (p - v)
        new_p = (
            node_cond * node_mirror(p)
            + current
            - slope * surface
            + plane_cond * (inner_plane(p) - ep)
        )
        new_v = collector_cond * (inner_plane(v) - ev) - node_mean(current)
        return new_p - shift * p, new_v - shift * v, current

    def shells_image(source, target, current, shift, dots=None, starts=()):
        images[source, 0] = images[source, 1]
        images[source, shells + 1] = images[source, shells]
        keep = (1.0 - shift)[None]

        def part(at, carry, last):
            here = images[source, pl.ds(at + 1, CHUNK)]
            low = images[source, pl.ds(at, CHUNK)]
            high = images[source, pl.ds(at + 2, CHUNK)]
            new = keep * here + diff[None] * (2.0 * here - low - high)
            if last:
                new = jnp.concatenate([new[:-1], new[-1:] + current[None]], axis=0)
            images[target, pl.ds(at + 1, CHUNK)] = new
            return tuple(dots(at, here, new, carry)) if dots else carry

        parts = shells // CHUNK
        carry = lax.fori_loop(
            0, parts - 1, lambda c, carry: part(c * CHUNK, carry, False), tuple(starts)
        )
        return part((parts - 1) * CHUNK, carry, True)

    def row_copy(step, px, py):
        return pltpu.make_async_remote_copy(
            src_ref=sent_rows.at[step],
            dst_ref=rows.at[step, me],
            send_sem=row_send.at[step],
            recv_sem=row_recv.at[step],
            device_id={"gx": px, "gy": py},
            device_id_type=MESH,
        )

    def send_dots(step, dots):
        padded = -(-len(dots) // 8) * 8
        stacked = [jnp.sum(d, axis=0, keepdims=True) for d in dots]
        stacked += [zero[:1]] * (padded - len(dots))
        tall = jnp.sum(jnp.concatenate(stacked, axis=0), axis=1, keepdims=True)
        at_row = lax.broadcasted_iota(jnp.int32, (padded, LANES), 0)
        at_lane = lax.broadcasted_iota(jnp.int32, (padded, LANES), 1)
        row = jnp.sum(jnp.where(at_row == at_lane, tall, 0.0), axis=0, keepdims=True)
        sent_rows[step] = row
        rows[step, me] = row
        peers(lambda px, py: row_copy(step, px, py).start())

    def wait_rows(step):
        part = rows.at[step, pl.ds(0, count - 1)]
        pltpu.make_async_copy(part, part, row_recv.at[step]).wait()

    def take_dots(step, wanted):
        total = jnp.sum(rows[step], axis=0)
        return [jnp.broadcast_to(total[:, k : k + 1], (subs, LANES)) for k in range(wanted)]

    pending = []

    def send_edges(slot, p, v):
        edges[slot, 0] = p
        edges[slot, 1] = v
        copies = edge_copies(slot)
        for copy in copies:
            copy.start()
        pending.extend(copies)
        return copies

    def take_edges(slot, copies, p, v):
        for copy in copies:
            copy.wait_recv()
        return p, v, edge_sum(slot, 0), edge_sum(slot, 1)

    def root(square):
        height = jnp.sqrt(square + epsilon)
        return height, 1.0 / height

    def ramp(square):
        return jnp.maximum(square, 0.0)

    def combine(coeffs, members):
        return add([c * m for c, m in zip(coeffs, members)])

    columns, cosines, sines, uppers, target = [], [], [], [], []

    def rotate():
        for step in range(len(uppers), len(columns)):
            entries = list(columns[step])
            for row in range(step):
                first = cosines[row] * entries[row] + sines[row] * entries[row + 1]
                second = cosines[row] * entries[row + 1] - sines[row] * entries[row]
                entries[row] = first
                entries[row + 1] = second
            square = entries[step] * entries[step] + entries[step + 1] * entries[step + 1]
            radius = jnp.sqrt(square)
            cosine = entries[step] / radius
            sine = entries[step + 1] / radius
            entries[step] = radius
            cosines.append(cosine)
            sines.append(sine)
            lead = target[step]
            target[step] = cosine * lead
            target.append(-sine * lead)
            uppers.append(entries[: step + 1])

    shift = jnp.full((subs, LANES), first_shift, jnp.float32)
    images_pots = [None, None, None]
    pl.semaphore_wait(barrier, count - 1)
    copies = send_edges(0, pot, vol)
    vecs = [take_edges(0, copies, pot, vol)]
    p, v, current = pots_image(vecs[0], images[2, shells], shift)
    copies = send_edges(1, p, v)

    def keep_first(at, here, new, carry):
        basis[0, pl.ds(at, CHUNK)] = here
        return carry

    shells_image(2, 0, current, shift, keep_first)
    images_pots[0] = take_edges(1, copies, p, v)
    p, v, current = pots_image(images_pots[0], images[0, shells], shift)
    slot = 2
    copies = send_edges(slot, p, v)
    gram = None
    for last in range(0, ITERS, 2):
        block = last // 2
        more = last + 2 < ITERS
        v_once = v * single
        z1 = images_pots[0]
        z1_once = z1[1] * single
        starts = [vecs[i][0] * z1[0] + vecs[i][1] * z1_once for i in range(last + 1)]
        starts += [vecs[i][0] * p + vecs[i][1] * v_once for i in range(last + 1)]
        starts += [z1[0] * z1[0] + z1[1] * z1_once]
        starts += [z1[0] * p + z1[1] * v_once, p * p + v * v_once]
        if block == 0:
            starts.append(pot * pot + vol * (vol * single))

        def dots(at, here, new, carry):
            others = [basis[i, pl.ds(at, CHUNK)] for i in range(last + 1)]
            out = [jnp.sum(q * here, axis=0) for q in others]
            out += [jnp.sum(q * new, axis=0) for q in others]
            out += [jnp.sum(m * n, axis=0) for m, n in ((here, here), (here, new), (new, new))]
            if block == 0:
                out.append(jnp.sum(others[0] * others[0], axis=0))
            return [c + o for c, o in zip(carry, out)]

        products = shells_image(0, 1, current, shift, dots, starts)
        send_dots(block, products)
        rotate()
        if more:
            images_pots[1] = take_edges(slot, copies, p, v)
            p, v, current = pots_image(images_pots[1], images[1, shells], shift)
            slot += 1
            copies = send_edges(slot, p, v)
            shells_image(1, 2, current, shift)
        wait_rows(block)
        sums = take_dots(block, len(products))
        scale = None
        if block == 0:
            beta, scale = root(sums[5])
            target.append(beta)
            sums = [s * scale * scale for s in sums]
            gram = [[sums[5]]]
        width = last + 1
        col1, col2, first, second, next_image, gram = two_columns(
            last,
            columns,
            gram,
            sums[:width],
            sums[width : 2 * width],
            sums[2 * width],
            sums[2 * width + 1],
            sums[2 * width + 2],
            shift,
            root,
            ramp,
        )
        columns += [col1, col2]
        if not more:
            break
        new_shift = col1[last]
        along, e1, e2, e3 = next_image(new_shift)
        one = first[0] + [first[1]]
        two = second[0] + [second[1], second[2]]
        three = along + [e1, e2, e3]
        shift = new_shift
        if block == 0:
            one, two, three = ([c * scale for c in cs] for cs in (one, two, three))
        images_pots[2] = take_edges(slot, copies, p, v)
        members = [list(m) for m in zip(*(vecs + images_pots))]
        new_vecs = [tuple(combine(cs, m) for m in members) for cs in (one, two, three)]
        if block == 0:
            vecs[0] = tuple(m * scale for m in vecs[0])
        vecs += new_vecs[:2]
        images_pots = [new_vecs[2], None, None]
        surfaces = [basis[i, shells - 1] for i in range(width)] + [
            images[k, shells] for k in range(3)
        ]
        p, v, current = pots_image(images_pots[0], combine(three, surfaces), shift)
        if last + 4 < ITERS:
            slot += 1
            copies = send_edges(slot, p, v)

        def advance(c, carry):
            at = c * CHUNK
            parts = [basis[i, pl.ds(at, CHUNK)] for i in range(width)]
            parts += [images[k, pl.ds(at + 1, CHUNK)] for k in range(3)]
            basis[last + 1, pl.ds(at, CHUNK)] = combine(one, parts)
            basis[last + 2, pl.ds(at, CHUNK)] = combine(two, parts)
            images[0, pl.ds(at + 1, CHUNK)] = combine(three, parts)
            if block == 0:
                basis[0, pl.ds(at, CHUNK)] = parts[0] * scale
            return carry

        lax.fori_loop(0, shells // CHUNK, advance, 0)
    rotate()

    weights = [None] * ITERS
    for row in range(ITERS - 1, -1, -1):
        total = target[row]
        for later in range(row + 1, ITERS):
            total = total - uppers[later][row] * weights[later]
        weights[row] = total / uppers[row][row]
    tail = weights[ITERS - 1]
    mixed = [weights[i] + tail * first[0][i] for i in range(ITERS - 1)] + [tail * first[1]]

    sol_p = combine(mixed, [m[0] for m in vecs] + [images_pots[0][0]])
    sol_v = combine(mixed, [m[1] for m in vecs] + [images_pots[0][1]])

    def gather(c, carry):
        at = c * CHUNK
        parts = [basis[i, pl.ds(at, CHUNK)] for i in range(ITERS - 1)]
        parts.append(images[0, pl.ds(at + 1, CHUNK)])
        images[1, pl.ds(at + 1, CHUNK)] = combine(mixed, parts)
        return carry

    lax.fori_loop(0, shells // CHUNK, gather, 0)
    flat = jnp.concatenate([images[1, 1 : shells + 1, s, :] for s in range(subs)], axis=0)
    turned[...] = flat.T
    for x in range(cx):
        for g in range(groups):
            edge_row = g * cells + x * cy
            sol_conc_ref[x, :, g * span : (g + 1) * span] = turned[edge_row : edge_row + cy, :]
    flat_p = jnp.concatenate(
        [sol_p[:, g * cells : (g + 1) * cells] for g in range(groups)] + [sol_v[:1, :cells]], axis=0
    )
    sol_pots_ref[...] = flat_p.T.reshape(cx, cy, nodes + 1)

    for copy in pending:
        copy.wait_send()
    for step in range(ITERS // 2):
        part = rows.at[step, pl.ds(0, count - 1)]
        pltpu.make_async_copy(part, part, row_send.at[step]).wait()


def solution(mesh):
    sizes = (mesh.shape["gx"], mesh.shape["gy"])
    count = sizes[0] * sizes[1]

    def shards(rhs_conc, rhs_pots, diffusion, exchange, slope):
        cells = rhs_conc.shape[0] * rhs_conc.shape[1]
        nodes = exchange.shape[2]
        shells = rhs_conc.shape[2] // nodes
        groups = LANES // cells
        subs = nodes // groups
        vmem = pl.BlockSpec(memory_space=pltpu.VMEM)
        return pl.pallas_call(
            functools.partial(cycle, sizes),
            out_shape=(
                jax.ShapeDtypeStruct(rhs_conc.shape, jnp.float32),
                jax.ShapeDtypeStruct(rhs_pots.shape, jnp.float32),
            ),
            in_specs=[vmem] * 5,
            out_specs=(vmem, vmem),
            scratch_shapes=[
                pltpu.VMEM((LANES, subs * shells), jnp.float32),
                pltpu.VMEM((ITERS - 1, shells, subs, LANES), jnp.float32),
                pltpu.VMEM((3, shells + 2, subs, LANES), jnp.float32),
                pltpu.VMEM((ITERS, 2, subs, LANES), jnp.float32),
                pltpu.VMEM((ITERS, 4, 2, subs, LANES), jnp.float32),
                pltpu.VMEM((ITERS // 2, count, 1, LANES), jnp.float32),
                pltpu.VMEM((ITERS // 2, 1, LANES), jnp.float32),
                pltpu.SemaphoreType.DMA((ITERS, 4)),
                pltpu.SemaphoreType.DMA((ITERS, 4)),
                pltpu.SemaphoreType.DMA((ITERS // 2,)),
                pltpu.SemaphoreType.DMA((ITERS // 2,)),
            ],
            compiler_params=pltpu.CompilerParams(collective_id=0, has_side_effects=True),
        )(rhs_conc, rhs_pots, diffusion, exchange, slope)

    spec = P("gx", "gy", None)
    return jax.shard_map(
        shards,
        mesh=mesh,
        in_specs=(spec,) * 5,
        out_specs=(spec, spec),
        check_vma=False,
    )
```

```python
import functools

import jax
import jax.numpy as jnp
from jax import lax
from jax.experimental import pallas as pl
from jax.experimental.pallas import tpu as pltpu
from jax.sharding import PartitionSpec as P

ITERS = 10
LANES = 128
CHUNK = 16

node_cond = 1.0
plane_cond = 0.5
collector_cond = 2.0
epsilon = 1e-06
first_shift = 3.0
MESH = pl.DeviceIdType.MESH


def add(terms):
    terms = [t for t in terms if t is not None]
    while len(terms) > 1:
        pairs = [terms[k] + terms[k + 1] for k in range(0, len(terms) - 1, 2)]
        terms = pairs + ([terms[-1]] if len(terms) % 2 else [])
    return terms[0]


def two_columns(last, upper, gram, along1, along2, z11, z12, z22, shift, root, ramp):
    span = range(last + 1)

    def images_of_rest(cu):
        out = []
        for k in span:
            terms = [cu[i] * upper[i][k] for i in range(max(k - 1, 0), last)]
            if k == last:
                terms.append(cu[last] * shift)
            out.append(add(terms))
        return out

    h = [along1[i] + shift * gram[i][last] for i in span]
    cu = [-h[i] for i in span]
    cu[last] = shift - h[last]
    gu = [h[i] - add([h[k] * gram[i][k] for k in span]) for i in span]
    g1 = z11 + shift * along1[last] - add([h[k] * along1[k] for k in span])
    g2 = z12 + shift * along2[last] - add([h[k] * along2[k] for k in span])
    square = add([cu[i] * gu[i] for i in span] + [g1])
    height, inverse = root(ramp(square))
    col1 = h + [height]
    first = [c * inverse for c in cu]
    near = [g * inverse for g in gu]
    near1, near2 = g1 * inverse, g2 * inverse
    near_self = ramp(square) * inverse * inverse

    cw = [c * inverse for c in images_of_rest(cu)]
    c1 = (cu[last] + shift) * inverse
    c2 = inverse
    g = [
        add([cw[k] * gram[i][k] for k in span] + [c1 * along1[i], c2 * along2[i]]) for i in span
    ]
    g1 = add([cw[k] * along1[k] for k in span] + [c1 * z11, c2 * z12])
    g2 = add([cw[k] * along2[k] for k in span] + [c1 * z12, c2 * z22])
    h = list(g)
    top = add([first[i] * g[i] for i in span] + [inverse * g1])
    cu = [cw[i] - h[i] - top * first[i] for i in span]
    c1 = c1 - top * inverse
    gu = [g[i] - add([h[k] * gram[i][k] for k in span] + [top * near[i]]) for i in span]
    g1 = g1 - add([h[k] * along1[k] for k in span] + [top * near1])
    g2 = g2 - add([h[k] * along2[k] for k in span] + [top * near2])
    square = add([cu[i] * gu[i] for i in span] + [c1 * g1, c2 * g2])
    height, inverse2 = root(ramp(square))
    col2 = h + [top, height]
    second = ([c * inverse2 for c in cu], c1 * inverse2, c2 * inverse2)

    def next_image(new_shift):
        cq, d1, d2 = second
        out = images_of_rest(cq)
        out = [out[k] - new_shift * cq[k] for k in span]
        e1 = cq[last] + d1 * (shift - new_shift)
        e2 = d1 + d2 * (shift - new_shift)
        return out, e1, e2, d2

    gram = [list(gram[i]) + [near[i], gu[i] * inverse2] for i in span]
    cross = add([first[i] * gu[i] for i in span] + [inverse * g1]) * inverse2
    gram.append([gram[i][last + 1] for i in span] + [near_self, cross])
    gram.append([gram[i][last + 2] for i in span] + [cross, ramp(square) * inverse2 * inverse2])
    return col1, col2, (first, inverse), second, next_image, gram


def cycle(
    sizes,
    conc_ref,
    pots_ref,
    diff_ref,
    exch_ref,
    slope_ref,
    sol_conc_ref,
    sol_pots_ref,
    turned,
    basis,
    images,
    edges,
    halos,
    rows,
    sent_rows,
    edge_send,
    edge_recv,
    row_send,
    row_recv,
):
    nx, ny = sizes
    count = nx * ny
    cx, cy = conc_ref.shape[0], conc_ref.shape[1]
    cells = cx * cy
    nodes = exch_ref.shape[2]
    shells = conc_ref.shape[2] // nodes
    groups = LANES // cells
    subs = nodes // groups
    mx = lax.axis_index("gx")
    my = lax.axis_index("gy")
    me = mx * ny + my

    def peers(act):
        if count <= 32:
            for dx in range(nx - 1, -1, -1):
                for dy in range(ny - 1, -1, -1):
                    if dx or dy:
                        act(lax.rem(mx + dx, nx), lax.rem(my + dy, ny))
        else:

            def one(p, carry):
                other = lax.rem(me + p, count)
                act(lax.div(other, ny), lax.rem(other, ny))
                return carry

            lax.fori_loop(1, count, one, 0)

    barrier = pltpu.get_barrier_semaphore()
    peers(
        lambda px, py: pl.semaphore_signal(
            barrier, inc=1, device_id={"gx": px, "gy": py}, device_id_type=MESH
        )
    )

    def fold_nodes(block):
        flat = block.reshape(cells, block.shape[2])
        return flat.T

    def node_register(flat_t):
        return jnp.concatenate(
            [flat_t[g * subs : (g + 1) * subs, :] for g in range(groups)], axis=1
        )

    diff = node_register(fold_nodes(diff_ref[...]))
    exch = node_register(fold_nodes(exch_ref[...]))
    slope = node_register(fold_nodes(slope_ref[...]))
    pots_t = fold_nodes(pots_ref[...])
    pot = node_register(pots_t)
    vol_row = pots_t[nodes : nodes + 1, :]
    vol = jnp.broadcast_to(jnp.concatenate([vol_row] * groups, axis=1), (subs, LANES))

    span = subs * shells
    for x in range(cx):
        for g in range(groups):
            edge_row = g * cells + x * cy
            turned[edge_row : edge_row + cy, :] = conc_ref[x, :, g * span : (g + 1) * span]
    turned_t = turned[...].T.reshape(subs, shells, LANES)
    for s in range(subs):
        images[2, 1 : shells + 1, s, :] = turned_t[s]

    lane = lax.broadcasted_iota(jnp.int32, (subs, LANES), 1)
    sub = lax.broadcasted_iota(jnp.int32, (subs, LANES), 0)
    group = lane // cells
    cell = lane % cells
    cell_x = cell // cy
    cell_y = cell % cy
    single = ((sub == 0) & (group == 0)).astype(jnp.float32)
    first_sub, last_sub = sub == 0, sub == subs - 1
    first_group, last_group = group == 0, group == groups - 1
    inside_low_x, inside_high_x = cell_x > 0, cell_x < cx - 1
    inside_low_y, inside_high_y = cell_y > 0, cell_y < cy - 1
    zero = jnp.zeros((subs, LANES), jnp.float32)
    has = [mx > 0, mx < nx - 1, my > 0, my < ny - 1]
    goes = [has[1], has[0], has[3], has[2]]

    def roll(value, shift, axis=1):
        shift = shift % value.shape[axis]
        return pltpu.roll(value, shift, axis) if shift else value

    def inner_plane(p):
        return (
            4.0 * p
            - jnp.where(inside_low_x, roll(p, cy), zero)
            - jnp.where(inside_high_x, roll(p, -cy), zero)
            - jnp.where(inside_low_y, roll(p, 1), zero)
            - jnp.where(inside_high_y, roll(p, -1), zero)
        )

    def edge_sum(slot, member):
        low_x = roll(halos[slot, 0, member], -(cx - 1) * cy)
        high_x = roll(halos[slot, 1, member], (cx - 1) * cy)
        low_y = roll(halos[slot, 2, member], -(cy - 1))
        high_y = roll(halos[slot, 3, member], cy - 1)
        return (
            jnp.where(~inside_low_x & has[0], low_x, zero)
            + jnp.where(~inside_high_x & has[1], high_x, zero)
            + jnp.where(~inside_low_y & has[2], low_y, zero)
            + jnp.where(~inside_high_y & has[3], high_y, zero)
        )

    def node_mirror(p):
        low = roll(p, 1, 0)
        inner = jnp.where(first_sub, jnp.where(first_group, p, roll(low, cells)), low)
        high = roll(p, -1, 0)
        outer = jnp.where(last_sub, jnp.where(last_group, p, roll(high, -cells)), high)
        return 2.0 * p - inner - outer

    def node_mean(value):
        total = jnp.broadcast_to(jnp.sum(value, axis=0, keepdims=True), (subs, LANES))
        shift = cells
        while shift < LANES:
            total = total + roll(total, shift)
            shift *= 2
        return total * (1.0 / nodes)

    def edge_copies(slot):
        copies = []
        targets = [
            (lax.rem(mx + 1, nx), my),
            (lax.rem(mx + nx - 1, nx), my),
            (mx, lax.rem(my + 1, ny)),
            (mx, lax.rem(my + ny - 1, ny)),
        ]
        for k, (px, py) in enumerate(targets):
            copies.append(
                pltpu.make_async_remote_copy(
                    src_ref=edges.at[slot],
                    dst_ref=halos.at[slot, k],
                    send_sem=edge_send.at[slot, k],
                    recv_sem=edge_recv.at[slot, k],
                    device_id={"gx": px, "gy": py},
                    device_id_type=MESH,
                )
            )
        return copies

    def pots_image(vec, surface, shift):
        p, v, ep, ev = vec
        current = exch * (p - v)
        new_p = (
            node_cond * node_mirror(p)
            + current
            - slope * surface
            + plane_cond * (inner_plane(p) - ep)
        )
        new_v = collector_cond * (inner_plane(v) - ev) - node_mean(current)
        return new_p - shift * p, new_v - shift * v, current

    def shells_image(source, target, current, shift, dots=None, starts=()):
        images[source, 0] = images[source, 1]
        images[source, shells + 1] = images[source, shells]
        keep = (1.0 - shift)[None]

        def part(at, carry, last):
            here = images[source, pl.ds(at + 1, CHUNK)]
            low = images[source, pl.ds(at, CHUNK)]
            high = images[source, pl.ds(at + 2, CHUNK)]
            new = keep * here + diff[None] * (2.0 * here - low - high)
            if last:
                new = jnp.concatenate([new[:-1], new[-1:] + current[None]], axis=0)
            images[target, pl.ds(at + 1, CHUNK)] = new
            return tuple(dots(at, here, new, carry)) if dots else carry

        parts = shells // CHUNK
        carry = lax.fori_loop(
            0, parts - 1, lambda c, carry: part(c * CHUNK, carry, False), tuple(starts)
        )
        return part((parts - 1) * CHUNK, carry, True)

    def row_copy(step, px, py):
        return pltpu.make_async_remote_copy(
            src_ref=sent_rows.at[step],
            dst_ref=rows.at[step, me],
            send_sem=row_send.at[step],
            recv_sem=row_recv.at[step],
            device_id={"gx": px, "gy": py},
            device_id_type=MESH,
        )

    def send_dots(step, dots):
        padded = -(-len(dots) // 8) * 8
        stacked = [jnp.sum(d, axis=0, keepdims=True) for d in dots]
        stacked += [zero[:1]] * (padded - len(dots))
        tall = jnp.sum(jnp.concatenate(stacked, axis=0), axis=1, keepdims=True)
        at_row = lax.broadcasted_iota(jnp.int32, (padded, LANES), 0)
        at_lane = lax.broadcasted_iota(jnp.int32, (padded, LANES), 1)
        row = jnp.sum(jnp.where(at_row == at_lane, tall, 0.0), axis=0, keepdims=True)
        sent_rows[step] = row
        rows[step, me] = row
        peers(lambda px, py: row_copy(step, px, py).start())

    def wait_rows(step):
        part = rows.at[step, pl.ds(0, count - 1)]
        pltpu.make_async_copy(part, part, row_recv.at[step]).wait()

    def take_dots(step, wanted):
        total = jnp.sum(rows[step], axis=0)
        return [jnp.broadcast_to(total[:, k : k + 1], (subs, LANES)) for k in range(wanted)]

    pending = []

    def send_edges(slot, p, v):
        edges[slot, 0] = p
        edges[slot, 1] = v
        copies = edge_copies(slot)
        for copy, there in zip(copies, goes):
            pl.when(there)(copy.start)
        pending.append(copies)
        return copies

    def take_edges(slot, copies, p, v):
        for copy, there in zip(copies, has):
            pl.when(there)(copy.wait_recv)
        return p, v, edge_sum(slot, 0), edge_sum(slot, 1)

    def root(square):
        height = jnp.sqrt(square + epsilon)
        return height, 1.0 / height

    def ramp(square):
        return jnp.maximum(square, 0.0)

    def combine(coeffs, members):
        return add([c * m for c, m in zip(coeffs, members)])

    columns, cosines, sines, uppers, target = [], [], [], [], []

    def rotate():
        for step in range(len(uppers), len(columns)):
            entries = list(columns[step])
            for row in range(step):
                first = cosines[row] * entries[row] + sines[row] * entries[row + 1]
                second = cosines[row] * entries[row + 1] - sines[row] * entries[row]
                entries[row] = first
                entries[row + 1] = second
            square = entries[step] * entries[step] + entries[step + 1] * entries[step + 1]
            radius = jnp.sqrt(square)
            cosine = entries[step] / radius
            sine = entries[step + 1] / radius
            entries[step] = radius
            cosines.append(cosine)
            sines.append(sine)
            lead = target[step]
            target[step] = cosine * lead
            target.append(-sine * lead)
            uppers.append(entries[: step + 1])

    shift = jnp.full((subs, LANES), first_shift, jnp.float32)
    images_pots = [None, None, None]
    pl.semaphore_wait(barrier, count - 1)
    copies = send_edges(0, pot, vol)
    vecs = [take_edges(0, copies, pot, vol)]
    p, v, current = pots_image(vecs[0], images[2, shells], shift)
    copies = send_edges(1, p, v)

    def keep_first(at, here, new, carry):
        basis[0, pl.ds(at, CHUNK)] = here
        return carry

    shells_image(2, 0, current, shift, keep_first)
    images_pots[0] = take_edges(1, copies, p, v)
    p, v, current = pots_image(images_pots[0], images[0, shells], shift)
    slot = 2
    copies = send_edges(slot, p, v)
    gram = None
    for last in range(0, ITERS, 2):
        block = last // 2
        more = last + 2 < ITERS
        v_once = v * single
        z1 = images_pots[0]
        z1_once = z1[1] * single
        starts = [vecs[i][0] * z1[0] + vecs[i][1] * z1_once for i in range(last + 1)]
        starts += [vecs[i][0] * p + vecs[i][1] * v_once for i in range(last + 1)]
        starts += [z1[0] * z1[0] + z1[1] * z1_once]
        starts += [z1[0] * p + z1[1] * v_once, p * p + v * v_once]
        if block == 0:
            starts.append(pot * pot + vol * (vol * single))

        def dots(at, here, new, carry):
            others = [basis[i, pl.ds(at, CHUNK)] for i in range(last + 1)]
            out = [jnp.sum(q * here, axis=0) for q in others]
            out += [jnp.sum(q * new, axis=0) for q in others]
            out += [jnp.sum(m * n, axis=0) for m, n in ((here, here), (here, new), (new, new))]
            if block == 0:
                out.append(jnp.sum(others[0] * others[0], axis=0))
            return [c + o for c, o in zip(carry, out)]

        products = shells_image(0, 1, current, shift, dots, starts)
        send_dots(block, products)
        rotate()
        if more:
            images_pots[1] = take_edges(slot, copies, p, v)
            p, v, current = pots_image(images_pots[1], images[1, shells], shift)
            slot += 1
            copies = send_edges(slot, p, v)
            shells_image(1, 2, current, shift)
        wait_rows(block)
        sums = take_dots(block, len(products))
        scale = None
        if block == 0:
            beta, scale = root(sums[5])
            target.append(beta)
            sums = [s * scale * scale for s in sums]
            gram = [[sums[5]]]
        width = last + 1
        col1, col2, first, second, next_image, gram = two_columns(
            last,
            columns,
            gram,
            sums[:width],
            sums[width : 2 * width],
            sums[2 * width],
            sums[2 * width + 1],
            sums[2 * width + 2],
            shift,
            root,
            ramp,
        )
        columns += [col1, col2]
        if not more:
            break
        new_shift = col1[last]
        along, e1, e2, e3 = next_image(new_shift)
        one = first[0] + [first[1]]
        two = second[0] + [second[1], second[2]]
        three = along + [e1, e2, e3]
        shift = new_shift
        if block == 0:
            one, two, three = ([c * scale for c in cs] for cs in (one, two, three))
        images_pots[2] = take_edges(slot, copies, p, v)
        members = [list(m) for m in zip(*(vecs + images_pots))]
        new_vecs = [tuple(combine(cs, m) for m in members) for cs in (one, two, three)]
        if block == 0:
            vecs[0] = tuple(m * scale for m in vecs[0])
        vecs += new_vecs[:2]
        images_pots = [new_vecs[2], None, None]
        surfaces = [basis[i, shells - 1] for i in range(width)] + [
            images[k, shells] for k in range(3)
        ]
        p, v, current = pots_image(images_pots[0], combine(three, surfaces), shift)
        if last + 4 < ITERS:
            slot += 1
            copies = send_edges(slot, p, v)

        def advance(c, carry):
            at = c * CHUNK
            parts = [basis[i, pl.ds(at, CHUNK)] for i in range(width)]
            parts += [images[k, pl.ds(at + 1, CHUNK)] for k in range(3)]
            basis[last + 1, pl.ds(at, CHUNK)] = combine(one, parts)
            basis[last + 2, pl.ds(at, CHUNK)] = combine(two, parts)
            images[0, pl.ds(at + 1, CHUNK)] = combine(three, parts)
            if block == 0:
                basis[0, pl.ds(at, CHUNK)] = parts[0] * scale
            return carry

        lax.fori_loop(0, shells // CHUNK, advance, 0)
    rotate()

    weights = [None] * ITERS
    for row in range(ITERS - 1, -1, -1):
        total = target[row]
        for later in range(row + 1, ITERS):
            total = total - uppers[later][row] * weights[later]
        weights[row] = total / uppers[row][row]
    tail = weights[ITERS - 1]
    mixed = [weights[i] + tail * first[0][i] for i in range(ITERS - 1)] + [tail * first[1]]

    sol_p = combine(mixed, [m[0] for m in vecs] + [images_pots[0][0]])
    sol_v = combine(mixed, [m[1] for m in vecs] + [images_pots[0][1]])

    def gather(c, carry):
        at = c * CHUNK
        parts = [basis[i, pl.ds(at, CHUNK)] for i in range(ITERS - 1)]
        parts.append(images[0, pl.ds(at + 1, CHUNK)])
        images[1, pl.ds(at + 1, CHUNK)] = combine(mixed, parts)
        return carry

    lax.fori_loop(0, shells // CHUNK, gather, 0)
    flat = jnp.concatenate([images[1, 1 : shells + 1, s, :] for s in range(subs)], axis=0)
    turned[...] = flat.T
    for x in range(cx):
        for g in range(groups):
            edge_row = g * cells + x * cy
            sol_conc_ref[x, :, g * span : (g + 1) * span] = turned[edge_row : edge_row + cy, :]
    flat_p = jnp.concatenate(
        [sol_p[:, g * cells : (g + 1) * cells] for g in range(groups)] + [sol_v[:1, :cells]], axis=0
    )
    sol_pots_ref[...] = flat_p.T.reshape(cx, cy, nodes + 1)

    for copies in pending:
        for copy, there in zip(copies, goes):
            pl.when(there)(copy.wait_send)
    for step in range(ITERS // 2):
        part = rows.at[step, pl.ds(0, count - 1)]
        pltpu.make_async_copy(part, part, row_send.at[step]).wait()


def solution(mesh):
    sizes = (mesh.shape["gx"], mesh.shape["gy"])
    count = sizes[0] * sizes[1]

    def shards(rhs_conc, rhs_pots, diffusion, exchange, slope):
        cells = rhs_conc.shape[0] * rhs_conc.shape[1]
        nodes = exchange.shape[2]
        shells = rhs_conc.shape[2] // nodes
        groups = LANES // cells
        subs = nodes // groups
        vmem = pl.BlockSpec(memory_space=pltpu.VMEM)
        return pl.pallas_call(
            functools.partial(cycle, sizes),
            out_shape=(
                jax.ShapeDtypeStruct(rhs_conc.shape, jnp.float32),
                jax.ShapeDtypeStruct(rhs_pots.shape, jnp.float32),
            ),
            in_specs=[vmem] * 5,
            out_specs=(vmem, vmem),
            scratch_shapes=[
                pltpu.VMEM((LANES, subs * shells), jnp.float32),
                pltpu.VMEM((ITERS - 1, shells, subs, LANES), jnp.float32),
                pltpu.VMEM((3, shells + 2, subs, LANES), jnp.float32),
                pltpu.VMEM((ITERS, 2, subs, LANES), jnp.float32),
                pltpu.VMEM((ITERS, 4, 2, subs, LANES), jnp.float32),
                pltpu.VMEM((ITERS // 2, count, 1, LANES), jnp.float32),
                pltpu.VMEM((ITERS // 2, 1, LANES), jnp.float32),
                pltpu.SemaphoreType.DMA((ITERS, 4)),
                pltpu.SemaphoreType.DMA((ITERS, 4)),
                pltpu.SemaphoreType.DMA((ITERS // 2,)),
                pltpu.SemaphoreType.DMA((ITERS // 2,)),
            ],
            compiler_params=pltpu.CompilerParams(collective_id=0, has_side_effects=True),
        )(rhs_conc, rhs_pots, diffusion, exchange, slope)

    spec = P("gx", "gy", None)
    return jax.shard_map(
        shards,
        mesh=mesh,
        in_specs=(spec,) * 5,
        out_specs=(spec, spec),
        check_vma=False,
    )
```

```python
import functools

import jax
import jax.numpy as jnp
from jax import lax
from jax.experimental import pallas as pl
from jax.experimental.pallas import tpu as pltpu
from jax.sharding import PartitionSpec as P

ITERS = 10
LANES = 128
CHUNK = 16

node_cond = 1.0
plane_cond = 0.5
collector_cond = 2.0
epsilon = 1e-06
first_shift = 3.0
MESH = pl.DeviceIdType.MESH


def add(terms):
    terms = [t for t in terms if t is not None]
    while len(terms) > 1:
        pairs = [terms[k] + terms[k + 1] for k in range(0, len(terms) - 1, 2)]
        terms = pairs + ([terms[-1]] if len(terms) % 2 else [])
    return terms[0]


def two_columns(last, upper, gram, along1, along2, z11, z12, z22, shift, root, ramp):
    span = range(last + 1)

    def images_of_rest(cu):
        out = []
        for k in span:
            terms = [cu[i] * upper[i][k] for i in range(max(k - 1, 0), last)]
            if k == last:
                terms.append(cu[last] * shift)
            out.append(add(terms))
        return out

    h = [along1[i] + shift * gram[i][last] for i in span]
    cu = [-h[i] for i in span]
    cu[last] = shift - h[last]
    gu = [h[i] - add([h[k] * gram[i][k] for k in span]) for i in span]
    g1 = z11 + shift * along1[last] - add([h[k] * along1[k] for k in span])
    g2 = z12 + shift * along2[last] - add([h[k] * along2[k] for k in span])
    square = add([cu[i] * gu[i] for i in span] + [g1])
    height, inverse = root(ramp(square))
    col1 = h + [height]
    first = [c * inverse for c in cu]
    near = [g * inverse for g in gu]
    near1, near2 = g1 * inverse, g2 * inverse
    near_self = ramp(square) * inverse * inverse

    cw = [c * inverse for c in images_of_rest(cu)]
    c1 = (cu[last] + shift) * inverse
    c2 = inverse
    g = [
        add([cw[k] * gram[i][k] for k in span] + [c1 * along1[i], c2 * along2[i]]) for i in span
    ]
    g1 = add([cw[k] * along1[k] for k in span] + [c1 * z11, c2 * z12])
    g2 = add([cw[k] * along2[k] for k in span] + [c1 * z12, c2 * z22])
    h = list(g)
    top = add([first[i] * g[i] for i in span] + [inverse * g1])
    cu = [cw[i] - h[i] - top * first[i] for i in span]
    c1 = c1 - top * inverse
    gu = [g[i] - add([h[k] * gram[i][k] for k in span] + [top * near[i]]) for i in span]
    g1 = g1 - add([h[k] * along1[k] for k in span] + [top * near1])
    g2 = g2 - add([h[k] * along2[k] for k in span] + [top * near2])
    square = add([cu[i] * gu[i] for i in span] + [c1 * g1, c2 * g2])
    height, inverse2 = root(ramp(square))
    col2 = h + [top, height]
    second = ([c * inverse2 for c in cu], c1 * inverse2, c2 * inverse2)

    def next_image(new_shift):
        cq, d1, d2 = second
        out = images_of_rest(cq)
        out = [out[k] - new_shift * cq[k] for k in span]
        e1 = cq[last] + d1 * (shift - new_shift)
        e2 = d1 + d2 * (shift - new_shift)
        return out, e1, e2, d2

    gram = [list(gram[i]) + [near[i], gu[i] * inverse2] for i in span]
    cross = add([first[i] * gu[i] for i in span] + [inverse * g1]) * inverse2
    gram.append([gram[i][last + 1] for i in span] + [near_self, cross])
    gram.append([gram[i][last + 2] for i in span] + [cross, ramp(square) * inverse2 * inverse2])
    return col1, col2, (first, inverse), second, next_image, gram


def cycle(
    sizes,
    conc_ref,
    pots_ref,
    diff_ref,
    exch_ref,
    slope_ref,
    sol_conc_ref,
    sol_pots_ref,
    turned,
    basis,
    images,
    edges,
    halos,
    rows,
    sent_rows,
    edge_send,
    edge_recv,
    row_send,
    row_recv,
    load_sem,
):
    nx, ny = sizes
    count = nx * ny
    cx, cy = conc_ref.shape[0], conc_ref.shape[1]
    cells = cx * cy
    nodes = exch_ref.shape[2]
    shells = conc_ref.shape[2] // nodes
    groups = LANES // cells
    subs = nodes // groups
    mx = lax.axis_index("gx")
    my = lax.axis_index("gy")
    me = mx * ny + my

    def peers(act):
        if count <= 32:
            for dx in range(nx - 1, -1, -1):
                for dy in range(ny - 1, -1, -1):
                    if dx or dy:
                        act(lax.rem(mx + dx, nx), lax.rem(my + dy, ny))
        else:

            def one(p, carry):
                other = lax.rem(me + p, count)
                act(lax.div(other, ny), lax.rem(other, ny))
                return carry

            lax.fori_loop(1, count, one, 0)

    barrier = pltpu.get_barrier_semaphore()
    peers(
        lambda px, py: pl.semaphore_signal(
            barrier, inc=1, device_id={"gx": px, "gy": py}, device_id_type=MESH
        )
    )

    span = subs * shells
    loads = []
    for x in range(cx):
        for g in range(groups):
            edge_row = g * cells + x * cy
            loads.append(
                pltpu.make_async_copy(
                    conc_ref.at[x, :, g * span : (g + 1) * span],
                    turned.at[edge_row : edge_row + cy, :],
                    load_sem.at[x, g],
                )
            )
    for copy in loads:
        copy.start()

    def fold_nodes(block):
        flat = block.reshape(cells, block.shape[2])
        return flat.T

    def node_register(flat_t):
        return jnp.concatenate(
            [flat_t[g * subs : (g + 1) * subs, :] for g in range(groups)], axis=1
        )

    diff = node_register(fold_nodes(diff_ref[...]))
    exch = node_register(fold_nodes(exch_ref[...]))
    slope = node_register(fold_nodes(slope_ref[...]))
    pots_t = fold_nodes(pots_ref[...])
    pot = node_register(pots_t)
    vol_row = pots_t[nodes : nodes + 1, :]
    vol = jnp.broadcast_to(jnp.concatenate([vol_row] * groups, axis=1), (subs, LANES))

    for copy in loads:
        copy.wait()
    turned_t = turned[...].T.reshape(subs, shells, LANES)
    for s in range(subs):
        images[2, 1 : shells + 1, s, :] = turned_t[s]

    lane = lax.broadcasted_iota(jnp.int32, (subs, LANES), 1)
    sub = lax.broadcasted_iota(jnp.int32, (subs, LANES), 0)
    group = lane // cells
    cell = lane % cells
    cell_x = cell // cy
    cell_y = cell % cy
    single = ((sub == 0) & (group == 0)).astype(jnp.float32)
    first_sub, last_sub = sub == 0, sub == subs - 1
    first_group, last_group = group == 0, group == groups - 1
    inside_low_x, inside_high_x = cell_x > 0, cell_x < cx - 1
    inside_low_y, inside_high_y = cell_y > 0, cell_y < cy - 1
    zero = jnp.zeros((subs, LANES), jnp.float32)
    has = [mx > 0, mx < nx - 1, my > 0, my < ny - 1]
    goes = [has[1], has[0], has[3], has[2]]

    def roll(value, shift, axis=1):
        shift = shift % value.shape[axis]
        return pltpu.roll(value, shift, axis) if shift else value

    def inner_plane(p):
        return (
            4.0 * p
            - jnp.where(inside_low_x, roll(p, cy), zero)
            - jnp.where(inside_high_x, roll(p, -cy), zero)
            - jnp.where(inside_low_y, roll(p, 1), zero)
            - jnp.where(inside_high_y, roll(p, -1), zero)
        )

    def edge_sum(slot, member):
        low_x = roll(halos[slot, 0, member], -(cx - 1) * cy)
        high_x = roll(halos[slot, 1, member], (cx - 1) * cy)
        low_y = roll(halos[slot, 2, member], -(cy - 1))
        high_y = roll(halos[slot, 3, member], cy - 1)
        return (
            jnp.where(~inside_low_x & has[0], low_x, zero)
            + jnp.where(~inside_high_x & has[1], high_x, zero)
            + jnp.where(~inside_low_y & has[2], low_y, zero)
            + jnp.where(~inside_high_y & has[3], high_y, zero)
        )

    def node_mirror(p):
        low = roll(p, 1, 0)
        inner = jnp.where(first_sub, jnp.where(first_group, p, roll(low, cells)), low)
        high = roll(p, -1, 0)
        outer = jnp.where(last_sub, jnp.where(last_group, p, roll(high, -cells)), high)
        return 2.0 * p - inner - outer

    def node_mean(value):
        total = jnp.broadcast_to(jnp.sum(value, axis=0, keepdims=True), (subs, LANES))
        shift = cells
        while shift < LANES:
            total = total + roll(total, shift)
            shift *= 2
        return total * (1.0 / nodes)

    def edge_copies(slot):
        copies = []
        targets = [
            (lax.rem(mx + 1, nx), my),
            (lax.rem(mx + nx - 1, nx), my),
            (mx, lax.rem(my + 1, ny)),
            (mx, lax.rem(my + ny - 1, ny)),
        ]
        for k, (px, py) in enumerate(targets):
            copies.append(
                pltpu.make_async_remote_copy(
                    src_ref=edges.at[slot],
                    dst_ref=halos.at[slot, k],
                    send_sem=edge_send.at[slot, k],
                    recv_sem=edge_recv.at[slot, k],
                    device_id={"gx": px, "gy": py},
                    device_id_type=MESH,
                )
            )
        return copies

    def pots_image(vec, surface, shift):
        p, v, ep, ev = vec
        current = exch * (p - v)
        new_p = (
            node_cond * node_mirror(p)
            + current
            - slope * surface
            + plane_cond * (inner_plane(p) - ep)
        )
        new_v = collector_cond * (inner_plane(v) - ev) - node_mean(current)
        return new_p - shift * p, new_v - shift * v, current

    def shells_image(source, target, current, shift, dots=None, starts=()):
        images[source, 0] = images[source, 1]
        images[source, shells + 1] = images[source, shells]
        keep = (1.0 - shift)[None]

        def part(at, carry, last):
            here = images[source, pl.ds(at + 1, CHUNK)]
            low = images[source, pl.ds(at, CHUNK)]
            high = images[source, pl.ds(at + 2, CHUNK)]
            new = keep * here + diff[None] * (2.0 * here - low - high)
            if last:
                new = jnp.concatenate([new[:-1], new[-1:] + current[None]], axis=0)
            images[target, pl.ds(at + 1, CHUNK)] = new
            return tuple(dots(at, here, new, carry)) if dots else carry

        parts = shells // CHUNK
        carry = lax.fori_loop(
            0, parts - 1, lambda c, carry: part(c * CHUNK, carry, False), tuple(starts)
        )
        return part((parts - 1) * CHUNK, carry, True)

    def row_copy(step, px, py):
        return pltpu.make_async_remote_copy(
            src_ref=sent_rows.at[step],
            dst_ref=rows.at[step, me],
            send_sem=row_send.at[step],
            recv_sem=row_recv.at[step],
            device_id={"gx": px, "gy": py},
            device_id_type=MESH,
        )

    def send_dots(step, dots):
        padded = -(-len(dots) // 8) * 8
        stacked = [jnp.sum(d, axis=0, keepdims=True) for d in dots]
        stacked += [zero[:1]] * (padded - len(dots))
        tall = jnp.sum(jnp.concatenate(stacked, axis=0), axis=1, keepdims=True)
        at_row = lax.broadcasted_iota(jnp.int32, (padded, LANES), 0)
        at_lane = lax.broadcasted_iota(jnp.int32, (padded, LANES), 1)
        row = jnp.sum(jnp.where(at_row == at_lane, tall, 0.0), axis=0, keepdims=True)
        sent_rows[step] = row
        rows[step, me] = row
        peers(lambda px, py: row_copy(step, px, py).start())

    def wait_rows(step):
        part = rows.at[step, pl.ds(0, count - 1)]
        pltpu.make_async_copy(part, part, row_recv.at[step]).wait()

    def take_dots(step, wanted):
        total = jnp.sum(rows[step], axis=0)
        return [jnp.broadcast_to(total[:, k : k + 1], (subs, LANES)) for k in range(wanted)]

    pending = []

    def send_edges(slot, p, v):
        edges[slot, 0] = p
        edges[slot, 1] = v
        copies = edge_copies(slot)
        for copy, there in zip(copies, goes):
            pl.when(there)(copy.start)
        pending.append(copies)
        return copies

    def take_edges(slot, copies, p, v):
        for copy, there in zip(copies, has):
            pl.when(there)(copy.wait_recv)
        return p, v, edge_sum(slot, 0), edge_sum(slot, 1)

    def root(square):
        height = jnp.sqrt(square + epsilon)
        return height, 1.0 / height

    def ramp(square):
        return jnp.maximum(square, 0.0)

    def combine(coeffs, members):
        return add([c * m for c, m in zip(coeffs, members)])

    columns, cosines, sines, uppers, target = [], [], [], [], []

    def rotate():
        for step in range(len(uppers), len(columns)):
            entries = list(columns[step])
            for row in range(step):
                first = cosines[row] * entries[row] + sines[row] * entries[row + 1]
                second = cosines[row] * entries[row + 1] - sines[row] * entries[row]
                entries[row] = first
                entries[row + 1] = second
            square = entries[step] * entries[step] + entries[step + 1] * entries[step + 1]
            radius = jnp.sqrt(square)
            cosine = entries[step] / radius
            sine = entries[step + 1] / radius
            entries[step] = radius
            cosines.append(cosine)
            sines.append(sine)
            lead = target[step]
            target[step] = cosine * lead
            target.append(-sine * lead)
            uppers.append(entries[: step + 1])

    shift = jnp.full((subs, LANES), first_shift, jnp.float32)
    images_pots = [None, None, None]
    pl.semaphore_wait(barrier, count - 1)
    copies = send_edges(0, pot, vol)
    vecs = [take_edges(0, copies, pot, vol)]
    p, v, current = pots_image(vecs[0], images[2, shells], shift)
    copies = send_edges(1, p, v)

    def keep_first(at, here, new, carry):
        basis[0, pl.ds(at, CHUNK)] = here
        return carry

    shells_image(2, 0, current, shift, keep_first)
    images_pots[0] = take_edges(1, copies, p, v)
    p, v, current = pots_image(images_pots[0], images[0, shells], shift)
    slot = 2
    copies = send_edges(slot, p, v)
    gram = None
    for last in range(0, ITERS, 2):
        block = last // 2
        more = last + 2 < ITERS
        v_once = v * single
        z1 = images_pots[0]
        z1_once = z1[1] * single
        starts = [vecs[i][0] * z1[0] + vecs[i][1] * z1_once for i in range(last + 1)]
        starts += [vecs[i][0] * p + vecs[i][1] * v_once for i in range(last + 1)]
        starts += [z1[0] * z1[0] + z1[1] * z1_once]
        starts += [z1[0] * p + z1[1] * v_once, p * p + v * v_once]
        if block == 0:
            starts.append(pot * pot + vol * (vol * single))

        def dots(at, here, new, carry):
            others = [basis[i, pl.ds(at, CHUNK)] for i in range(last + 1)]
            out = [jnp.sum(q * here, axis=0) for q in others]
            out += [jnp.sum(q * new, axis=0) for q in others]
            out += [jnp.sum(m * n, axis=0) for m, n in ((here, here), (here, new), (new, new))]
            if block == 0:
                out.append(jnp.sum(others[0] * others[0], axis=0))
            return [c + o for c, o in zip(carry, out)]

        products = shells_image(0, 1, current, shift, dots, starts)
        send_dots(block, products)
        rotate()
        if more:
            images_pots[1] = take_edges(slot, copies, p, v)
            p, v, current = pots_image(images_pots[1], images[1, shells], shift)
            slot += 1
            copies = send_edges(slot, p, v)
            shells_image(1, 2, current, shift)
        wait_rows(block)
        sums = take_dots(block, len(products))
        scale = None
        if block == 0:
            beta, scale = root(sums[5])
            target.append(beta)
            sums = [s * scale * scale for s in sums]
            gram = [[sums[5]]]
        width = last + 1
        col1, col2, first, second, next_image, gram = two_columns(
            last,
            columns,
            gram,
            sums[:width],
            sums[width : 2 * width],
            sums[2 * width],
            sums[2 * width + 1],
            sums[2 * width + 2],
            shift,
            root,
            ramp,
        )
        columns += [col1, col2]
        if not more:
            break
        new_shift = col1[last]
        along, e1, e2, e3 = next_image(new_shift)
        one = first[0] + [first[1]]
        two = second[0] + [second[1], second[2]]
        three = along + [e1, e2, e3]
        shift = new_shift
        if block == 0:
            one, two, three = ([c * scale for c in cs] for cs in (one, two, three))
        images_pots[2] = take_edges(slot, copies, p, v)
        members = [list(m) for m in zip(*(vecs + images_pots))]
        new_vecs = [tuple(combine(cs, m) for m in members) for cs in (one, two, three)]
        if block == 0:
            vecs[0] = tuple(m * scale for m in vecs[0])
        vecs += new_vecs[:2]
        images_pots = [new_vecs[2], None, None]
        surfaces = [basis[i, shells - 1] for i in range(width)] + [
            images[k, shells] for k in range(3)
        ]
        p, v, current = pots_image(images_pots[0], combine(three, surfaces), shift)
        if last + 4 < ITERS:
            slot += 1
            copies = send_edges(slot, p, v)

        def advance(c, carry):
            at = c * CHUNK
            parts = [basis[i, pl.ds(at, CHUNK)] for i in range(width)]
            parts += [images[k, pl.ds(at + 1, CHUNK)] for k in range(3)]
            basis[last + 1, pl.ds(at, CHUNK)] = combine(one, parts)
            basis[last + 2, pl.ds(at, CHUNK)] = combine(two, parts)
            images[0, pl.ds(at + 1, CHUNK)] = combine(three, parts)
            if block == 0:
                basis[0, pl.ds(at, CHUNK)] = parts[0] * scale
            return carry

        lax.fori_loop(0, shells // CHUNK, advance, 0)
    rotate()

    weights = [None] * ITERS
    for row in range(ITERS - 1, -1, -1):
        total = target[row]
        for later in range(ITERS - 1, row, -1):
            total = total - uppers[later][row] * weights[later]
        weights[row] = total * (1.0 / uppers[row][row])
    tail = weights[ITERS - 1]
    mixed = [weights[i] + tail * first[0][i] for i in range(ITERS - 1)] + [tail * first[1]]

    sol_p = combine(mixed, [m[0] for m in vecs] + [images_pots[0][0]])
    sol_v = combine(mixed, [m[1] for m in vecs] + [images_pots[0][1]])

    def gather(c, carry):
        at = c * CHUNK
        parts = [basis[i, pl.ds(at, CHUNK)] for i in range(ITERS - 1)]
        parts.append(images[0, pl.ds(at + 1, CHUNK)])
        images[1, pl.ds(at + 1, CHUNK)] = combine(mixed, parts)
        return carry

    lax.fori_loop(0, shells // CHUNK, gather, 0)
    flat = jnp.concatenate([images[1, 1 : shells + 1, s, :] for s in range(subs)], axis=0)
    turned[...] = flat.T
    for x in range(cx):
        for g in range(groups):
            edge_row = g * cells + x * cy
            sol_conc_ref[x, :, g * span : (g + 1) * span] = turned[edge_row : edge_row + cy, :]
    flat_p = jnp.concatenate(
        [sol_p[:, g * cells : (g + 1) * cells] for g in range(groups)] + [sol_v[:1, :cells]], axis=0
    )
    sol_pots_ref[...] = flat_p.T.reshape(cx, cy, nodes + 1)

    for copies in pending:
        for copy, there in zip(copies, goes):
            pl.when(there)(copy.wait_send)
    for step in range(ITERS // 2):
        part = rows.at[step, pl.ds(0, count - 1)]
        pltpu.make_async_copy(part, part, row_send.at[step]).wait()


def solution(mesh):
    sizes = (mesh.shape["gx"], mesh.shape["gy"])
    count = sizes[0] * sizes[1]

    def shards(rhs_conc, rhs_pots, diffusion, exchange, slope):
        cells = rhs_conc.shape[0] * rhs_conc.shape[1]
        nodes = exchange.shape[2]
        shells = rhs_conc.shape[2] // nodes
        groups = LANES // cells
        subs = nodes // groups
        vmem = pl.BlockSpec(memory_space=pltpu.VMEM)
        return pl.pallas_call(
            functools.partial(cycle, sizes),
            out_shape=(
                jax.ShapeDtypeStruct(rhs_conc.shape, jnp.float32),
                jax.ShapeDtypeStruct(rhs_pots.shape, jnp.float32),
            ),
            in_specs=[pl.BlockSpec(memory_space=pl.ANY)] + [vmem] * 4,
            out_specs=(vmem, vmem),
            scratch_shapes=[
                pltpu.VMEM((LANES, subs * shells), jnp.float32),
                pltpu.VMEM((ITERS - 1, shells, subs, LANES), jnp.float32),
                pltpu.VMEM((3, shells + 2, subs, LANES), jnp.float32),
                pltpu.VMEM((ITERS, 2, subs, LANES), jnp.float32),
                pltpu.VMEM((ITERS, 4, 2, subs, LANES), jnp.float32),
                pltpu.VMEM((ITERS // 2, count, 1, LANES), jnp.float32),
                pltpu.VMEM((ITERS // 2, 1, LANES), jnp.float32),
                pltpu.SemaphoreType.DMA((ITERS, 4)),
                pltpu.SemaphoreType.DMA((ITERS, 4)),
                pltpu.SemaphoreType.DMA((ITERS // 2,)),
                pltpu.SemaphoreType.DMA((ITERS // 2,)),
                pltpu.SemaphoreType.DMA((rhs_conc.shape[0], groups)),
            ],
            compiler_params=pltpu.CompilerParams(collective_id=0, has_side_effects=True),
        )(rhs_conc, rhs_pots, diffusion, exchange, slope)

    spec = P("gx", "gy", None)
    return jax.shard_map(
        shards,
        mesh=mesh,
        in_specs=(spec,) * 5,
        out_specs=(spec, spec),
        check_vma=False,
    )
```
